32 devices in a mesh: gx: 8 (over z, x), gy: 4 (over y, core).
Axes of the slice: x: 2, y: 2, z: 4, core: 2. Of those that a mesh axis runs over, the one named last changes fastest.
Arguments:
- inputs: bfloat16 [4096, 1536], P('gx'), may hold values from -48 to 48
- gain_attn: bfloat16 [2, 1536], P(None, 'gx'), may hold values from 0.25 to 1.75
- w_query: bfloat16 [2, 1536, 1536], P(None, 'gx', 'gy'), may hold values from -0.15625 to 0.15625
- w_key: bfloat16 [2, 1536, 768], P(None, 'gx', 'gy'), may hold values from -0.15625 to 0.15625
- value_projection: bfloat16 [2, 1536, 768], P(None, 'gx', 'gy'), may hold values from -0.15625 to 0.15625
- w_out: bfloat16 [2, 1536, 1536], P(None, 'gy', 'gx'), may hold values from -1.75 to 1.75
- gain_ffn: bfloat16 [2, 1536], P(None, 'gx'), may hold values from 0.25 to 1.75
- w_gate: bfloat16 [2, 1536, 4096], P(None, 'gx', 'gy'), may hold values from -0.15625 to 0.15625
- w_up: bfloat16 [2, 1536, 4096], P(None, 'gx', 'gy'), may hold values from -0.15625 to 0.15625
- w_down: bfloat16 [2, 4096, 1536], P(None, 'gy', 'gx'), may hold values from -0.09375 to 0.09375
- cotangent: float32 [4096, 1536], P('gx'), may hold values from -6 to 6
Outputs:
- result: float32 [4096, 1536], P('gx')
- grad_inputs: float32 [4096, 1536], P('gx')
- grad_gain_attn: float32 [2, 1536], P(None, 'gx')
- grad_w_query: float32 [2, 1536, 1536], P(None, 'gx', 'gy')
- grad_w_key: float32 [2, 1536, 768], P(None, 'gx', 'gy')
- grad_w_value: float32 [2, 1536, 768], P(None, 'gx', 'gy')
- grad_w_out: float32 [2, 1536, 1536], P(None, 'gy', 'gx')
- grad_gain_ffn: float32 [2, 1536], P(None, 'gx')
- grad_w_gate: float32 [2, 1536, 4096], P(None, 'gx', 'gy')
- grad_w_up: float32 [2, 1536, 4096], P(None, 'gx', 'gy')
- grad_w_down: float32 [2, 4096, 1536], P(None, 'gy', 'gx')
The draws below stay inside these ranges and needn't reach their ends.
All inputs are finite; a program needn't handle non-finite values.
Results may differ from the reference program's by a relative error of at most 0.025.
Values may be sent and summed in bfloat16 or wider, within the bound.
A program may use at most 256 MiB of HBM per device.

```python
import math
import jax
import jax.numpy as jnp
from jax import lax

MODEL_WIDTH = 1536
QUERY_HEADS = 16
KEY_VALUE_HEADS = 8
HEAD_SIZE = 96
FF = 4096
DECODER_LAYERS = 2
P_SIZE = 128
SEQS = 4
TOKEN_COUNT = 4096
N_GX = 8


def draw_inputs(key, part):
    row_index = jnp.arange(TOKEN_COUNT, dtype=jnp.int32)[:, None]
    col_index = jnp.arange(MODEL_WIDTH, dtype=jnp.int32)[None, :]
    blocks = TOKEN_COUNT // (SEQS * P_SIZE)
    block_width = MODEL_WIDTH // blocks
    pairing = jax.random.permutation(jax.random.fold_in(key, 3), blocks)
    paired = pairing[row_index // (SEQS * P_SIZE)] == col_index // block_width
    spike_factor = jnp.where(paired, 3.0, 1.0)
    low_log = math.log(0.3)
    high_log = math.log(3.0)
    row_scale = jnp.exp(jax.random.uniform(jax.random.fold_in(key, 1), (TOKEN_COUNT, 1), jnp.float32, low_log, high_log))
    col_scale = jnp.exp(jax.random.uniform(jax.random.fold_in(key, 2), (1, MODEL_WIDTH), jnp.float32, low_log, high_log))
    base_values = jax.random.normal(jax.random.fold_in(key, 0), (TOKEN_COUNT, MODEL_WIDTH), jnp.float32)
    values = base_values * row_scale * col_scale * spike_factor
    return jnp.clip(values, -48.0, 48.0).astype(jnp.bfloat16)


def spiked(drawn, own_key, source, target, blocks, factor):
    owner, partner = [(jnp.arange(drawn.shape[axis_at]) // (drawn.shape[axis_at] // blocks)).reshape([-1 if axis == axis_at else 1 for axis in range(drawn.ndim)]) for axis_at in (source, target)]
    chosen = jax.random.permutation(own_key, blocks)[partner]
    strong = (owner == chosen) | (owner == (partner + blocks // 2) % blocks)
    return jnp.where(strong, factor * drawn, drawn)


def steps_of(key, dims, pieces, low, largest):
    factor_of = 1.0
    for dim, parts in pieces:
        draws = jax.random.uniform(jax.random.fold_in(jax.random.fold_in(key, 6), dim), (parts,), jnp.float32, low / len(pieces), largest / len(pieces))
        factor_of = factor_of * jnp.repeat(jnp.exp(draws), dims[dim] // parts).reshape((-1,) + (1,) * (len(dims) - 1 - dim))
    return factor_of


def scatter_about(key, dims, scale, bound, pieces=(), kind=jnp.bfloat16):
    drawn = scale * jax.random.normal(key, dims, jnp.float32)
    if pieces:
        drawn = drawn * steps_of(key, dims, pieces, -0.22, 0.18)
    return jnp.clip(drawn, -bound, bound).astype(kind)


def heavy_noise(stream_key, dims, spread, most, pieces, heavy, held_as=jnp.bfloat16):
    drawn = spread * jax.random.normal(stream_key, dims, jnp.float32)
    if pieces:
        drawn = drawn * steps_of(stream_key, dims, pieces, -0.22, 0.18)
    return jnp.clip(spiked(drawn, jax.random.fold_in(stream_key, 3), *heavy), -most, most).astype(held_as)


def setup_inputs(seed: int = 0) -> dict:
    key_of = jax.random.split(jax.random.key(seed), 12)
    return {
        "inputs": draw_inputs(jax.random.fold_in(key_of[11], 71), 0),
        "gain_attn": jnp.clip(1.0 + 0.15 * jax.random.normal(key_of[1], (DECODER_LAYERS, MODEL_WIDTH), jnp.float32), 0.25, 1.75).astype(jnp.bfloat16),
        "w_query": scatter_about(key_of[2], (DECODER_LAYERS, MODEL_WIDTH, QUERY_HEADS * HEAD_SIZE), MODEL_WIDTH ** -0.5, 0.15625, ((1, 8), (2, 4))),
        "w_key": scatter_about(key_of[3], (DECODER_LAYERS, MODEL_WIDTH, KEY_VALUE_HEADS * HEAD_SIZE), MODEL_WIDTH ** -0.5, 0.15625, ((1, 8), (2, 4))),
        "value_projection": scatter_about(key_of[4], (DECODER_LAYERS, MODEL_WIDTH, KEY_VALUE_HEADS * HEAD_SIZE), MODEL_WIDTH ** -0.5, 0.15625, ((1, 8), (2, 4))),
        "w_out": scatter_about(key_of[5], (DECODER_LAYERS, QUERY_HEADS * HEAD_SIZE, MODEL_WIDTH), (max(1, QUERY_HEADS * HEAD_SIZE * 8 // (P_SIZE * N_GX))) ** -0.5, 1.75, ((1, 4), (2, 8))),
        "gain_ffn": jnp.clip(1.0 + 0.15 * jax.random.normal(key_of[6], (DECODER_LAYERS, MODEL_WIDTH), jnp.float32), 0.25, 1.75).astype(jnp.bfloat16),
        "w_gate": scatter_about(key_of[7], (DECODER_LAYERS, MODEL_WIDTH, FF), MODEL_WIDTH ** -0.5, 0.15625, ((1, 8), (2, 4))),
        "w_up": scatter_about(key_of[8], (DECODER_LAYERS, MODEL_WIDTH, FF), MODEL_WIDTH ** -0.5, 0.15625, ((1, 8), (2, 4))),
        "w_down": scatter_about(key_of[9], (DECODER_LAYERS, FF, MODEL_WIDTH), FF ** -0.5, 0.09375, ((1, 4), (2, 8))),
        "cotangent": heavy_noise(key_of[10], (TOKEN_COUNT, MODEL_WIDTH), 1.0, 6.0, ((0, 8),), (0, 1, 8, 2.0), jnp.float32),
    }


@jax.custom_vjp
def reduced_precision(v):
    return lax.optimization_barrier(v.astype(jnp.bfloat16)).astype(jnp.float32)

@jax.custom_vjp
def low_back(v):
    return v

def low_keep(v):
    return (reduced_precision(v), None)

def low_pass(kept, grad):
    return (grad,)

def back_keep(v):
    return (v, None)

def back_low(kept, grad):
    return (reduced_precision(grad),)
reduced_precision.defvjp(low_keep, low_pass)
low_back.defvjp(back_keep, back_low)
norm_eps = 1e-05
rope_base = 100000.0
big_negative = -1e+30
highest = lax.Precision.HIGHEST

def rope_tables(positions, head_dim):
    half_dim = head_dim // 2
    exponents = jnp.arange(half_dim, dtype=jnp.float32) * (2.0 / head_dim)
    frequency = rope_base ** (-exponents)
    angles = positions[:, None] * frequency[None, :]
    return (jnp.cos(angles), jnp.sin(angles))

def apply_rotary(values, cosine_table, sine_table):
    half_dim = values.shape[-1] // 2
    first = values[..., :half_dim]
    second = values[..., half_dim:]
    cos_rows = cosine_table[:, None, :]
    sin_rows = sine_table[:, None, :]
    return jnp.concatenate([first * cos_rows - second * sin_rows, second * cos_rows + first * sin_rows], axis=-1)

def rms_norm(hidden, gain):
    factor = lax.rsqrt(lax.optimization_barrier(jnp.mean(hidden * hidden, axis=-1, keepdims=True)) + norm_eps)
    return hidden * factor * gain

def split_sequences(array):
    trailing = array.shape[1:]
    grouped = array.reshape((N_GX, SEQS, P_SIZE) + trailing)
    return jnp.swapaxes(grouped, 0, 1).reshape((SEQS, N_GX * P_SIZE) + trailing)

def from_sequences(array):
    trailing = array.shape[2:]
    grouped = array.reshape((SEQS, N_GX, P_SIZE) + trailing)
    return jnp.swapaxes(grouped, 0, 1).reshape((TOKEN_COUNT,) + trailing)

def attend_sequence(queries, keys, values):
    length = queries.shape[0]
    block_rows = min(512, length)
    block_count = length // block_rows
    key_pos = jnp.arange(length, dtype=jnp.int32)
    inv_sqrt = HEAD_SIZE ** (-0.5)

    def one_block(packed):
        block_query, first_row = packed
        scores = jnp.einsum('qkgd,tkd->kgqt', block_query, keys, precision=highest) * inv_sqrt
        scores = low_back(scores)
        query_pos = first_row + jnp.arange(block_rows, dtype=jnp.int32)
        allowed = key_pos[None, :] <= query_pos[:, None]
        scores = jnp.where(allowed, scores, big_negative)
        row_max = lax.optimization_barrier(jnp.max(scores, axis=-1, keepdims=True))
        expo = jnp.exp(scores - row_max)
        probs = reduced_precision(expo / lax.optimization_barrier(jnp.sum(expo, axis=-1, keepdims=True)))
        return jnp.einsum('kgqt,tkd->qkgd', probs, values, precision=highest)
    blocks = queries.reshape((block_count, block_rows) + queries.shape[1:])
    firsts = (jnp.arange(block_count, dtype=jnp.int32) * block_rows).astype(jnp.int32)
    outcome = lax.map(jax.checkpoint(one_block), (blocks, firsts))
    return outcome.reshape(queries.shape)

def reference(inputs, gain_attn, w_query, w_key, value_projection, w_out, gain_ffn, w_gate, w_up, w_down, cotangent):
    query_groups = QUERY_HEADS // KEY_VALUE_HEADS
    row_index = jnp.arange(TOKEN_COUNT, dtype=jnp.int32)
    positions = (row_index // (SEQS * P_SIZE) * P_SIZE + row_index % P_SIZE).astype(jnp.float32)
    cosine_table, sine_table = rope_tables(positions, HEAD_SIZE)

    def layer(hidden, weights):
        attn_gain, query_mat, key_mat, value_mat, out_mat, ffn_gain, gate_mat, up_mat, down_mat = weights
        normed = reduced_precision(rms_norm(hidden, attn_gain))
        query_lin = low_back(jnp.dot(normed, query_mat, precision=highest))
        key_linear = low_back(jnp.dot(normed, key_mat, precision=highest))
        value_reduced = low_back(reduced_precision(jnp.dot(normed, value_mat, precision=highest)))
        query_rotated = reduced_precision(apply_rotary(query_lin.reshape(TOKEN_COUNT, QUERY_HEADS, HEAD_SIZE), cosine_table, sine_table))
        key_rotated = reduced_precision(apply_rotary(key_linear.reshape(TOKEN_COUNT, KEY_VALUE_HEADS, HEAD_SIZE), cosine_table, sine_table))
        query_sequence = split_sequences(query_rotated.reshape(TOKEN_COUNT, KEY_VALUE_HEADS, query_groups, HEAD_SIZE))
        key_seq = split_sequences(key_rotated)
        value_sequence = split_sequences(value_reduced.reshape(TOKEN_COUNT, KEY_VALUE_HEADS, HEAD_SIZE))
        attended = lax.map(lambda packed: attend_sequence(packed[0], packed[1], packed[2]), (query_sequence, key_seq, value_sequence))
        mixed = low_back(reduced_precision(from_sequences(attended).reshape(TOKEN_COUNT, QUERY_HEADS * HEAD_SIZE)))
        middle = hidden + low_back(jnp.dot(mixed, out_mat, precision=highest))
        normed_ffn = reduced_precision(rms_norm(middle, ffn_gain))
        gate = low_back(jnp.dot(normed_ffn, gate_mat, precision=highest))
        upward = low_back(jnp.dot(normed_ffn, up_mat, precision=highest))
        inner = reduced_precision(jax.nn.silu(gate) * upward)
        return middle + low_back(jnp.dot(inner, down_mat, precision=highest))

    def forward(first_input, attn_gains, query_mats, key_mats, value_mats, out_mats, ffn_gains, gate_mats, up_mats, down_mats):
        hidden = first_input
        for layer_index in range(DECODER_LAYERS):
            hidden = layer(hidden, (attn_gains[layer_index], query_mats[layer_index], key_mats[layer_index], value_mats[layer_index], out_mats[layer_index], ffn_gains[layer_index], gate_mats[layer_index], up_mats[layer_index], down_mats[layer_index]))
        return hidden
    arrays = (inputs, gain_attn, w_query, w_key, value_projection, w_out, gain_ffn, w_gate, w_up, w_down)
    arrays = tuple((item.astype(jnp.float32) for item in arrays))
    result, pullback = jax.vjp(forward, *arrays)
    grads = pullback(cotangent.astype(jnp.float32))
    return (result, grads[0], grads[1], grads[2], grads[3], grads[4], grads[5], grads[6], grads[7], grads[8], grads[9])
```

```python
import jax
import jax.numpy as jnp
from jax import lax
from jax.sharding import PartitionSpec as P

QUERY_HEADS = 16
KEY_VALUE_HEADS = 8
HEAD_SIZE = 96
DECODER_LAYERS = 2
P_SIZE = 128

norm_eps = 1e-05
rope_base = 100000.0
big_negative = -1e30
F32 = jnp.float32
BF16 = jnp.bfloat16

def rope_tables(positions, head_dim):
    half_dim = head_dim // 2
    exponents = jnp.arange(half_dim, dtype=jnp.float32) * (2.0 / head_dim)
    frequency = rope_base ** (-exponents)
    angles = positions[:, None] * frequency[None, :]
    return (jnp.cos(angles), jnp.sin(angles))


def apply_rotary(values, cosine_table, sine_table):
    half_dim = values.shape[-1] // 2
    first = values[..., :half_dim]
    second = values[..., half_dim:]
    cos_rows = cosine_table[:, None, :]
    sin_rows = sine_table[:, None, :]
    return jnp.concatenate(
        [first * cos_rows - second * sin_rows, second * cos_rows + first * sin_rows], axis=-1
    )


def rotate_back(grads, cosine_table, sine_table):
    half_dim = grads.shape[-1] // 2
    first = grads[..., :half_dim]
    second = grads[..., half_dim:]
    cos_rows = cosine_table[:, None, :]
    sin_rows = sine_table[:, None, :]
    return jnp.concatenate(
        [first * cos_rows + second * sin_rows, second * cos_rows - first * sin_rows], axis=-1
    )


def key_slab(kv_all, block, key_block, queries):
    seq_count, piece_len, kv_heads, query_groups, head_dim = queries.shape
    row_count = seq_count * piece_len
    slab = lax.dynamic_slice_in_dim(
        kv_all, block * (key_block * row_count), key_block * row_count, 0
    )
    slab = slab.reshape(key_block, seq_count, piece_len, 2, kv_heads, head_dim)
    slab = jnp.transpose(slab, (1, 0, 2, 3, 4, 5)).reshape(
        seq_count, key_block * piece_len, 2, kv_heads, head_dim
    )
    return (slab[:, :, 0], slab[:, :, 1])


def masked_scores(queries, keys, block, piece, key_block):
    piece_len = queries.shape[1]
    head_dim = queries.shape[4]
    key_len = key_block * piece_len
    query_pos = piece * piece_len + jnp.arange(piece_len, dtype=jnp.int32)
    key_pos = block * key_len + jnp.arange(key_len, dtype=jnp.int32)
    allowed = key_pos[None, :] <= query_pos[:, None]
    raw = jnp.einsum(
        "spkgd,stkd->skgpt", queries, keys, preferred_element_type=jnp.float32
    ) * head_dim ** (-0.5)
    return jnp.where(allowed, raw, big_negative)


def attend_forward(queries, kv_all, piece, key_block):
    seq_count, piece_len, kv_heads, query_groups, head_dim = queries.shape

    def step(block, carry):
        run_max, run_sum, total = carry
        keys, values = key_slab(kv_all, block, key_block, queries)
        scores = masked_scores(queries, keys, block, piece, key_block)
        new_max = jnp.maximum(run_max, jnp.max(scores, axis=-1))
        factor = jnp.exp(run_max - new_max)
        expo = jnp.exp(scores - new_max[..., None])
        run_sum = run_sum * factor + jnp.sum(expo, axis=-1)
        total = total * factor[..., None] + jnp.einsum(
            "skgpt,stkd->skgpd",
            expo.astype(jnp.bfloat16),
            values,
            preferred_element_type=jnp.float32,
        )
        return (new_max, run_sum, total)

    stats_shape = (seq_count, kv_heads, query_groups, piece_len)
    start = (
        jnp.full(stats_shape, big_negative, jnp.float32),
        jnp.zeros(stats_shape, jnp.float32),
        jnp.zeros(stats_shape + (head_dim,), jnp.float32),
    )
    run_max, run_sum, total = lax.fori_loop(0, piece // key_block + 1, step, start)
    return (total / run_sum[..., None], run_max + jnp.log(run_sum))


def attend_backward(queries, kv_all, piece, key_block, log_total, grad_heads, delta_rows, pieces):
    seq_count, piece_len, kv_heads, query_groups, head_dim = queries.shape
    row_count = seq_count * piece_len
    inv_sqrt = head_dim ** (-0.5)

    def step(block, carry):
        grad_query, terms = carry
        keys, values = key_slab(kv_all, block, key_block, queries)
        probs = jnp.exp(
            masked_scores(queries, keys, block, piece, key_block) - log_total[..., None]
        )
        grad_values = jnp.einsum(
            "skgpt,skgpd->stkd",
            probs.astype(jnp.bfloat16),
            grad_heads,
            preferred_element_type=jnp.float32,
        )
        grad_probs = jnp.einsum(
            "skgpd,stkd->skgpt", grad_heads, values, preferred_element_type=jnp.float32
        )
        grad_scores = (probs * (grad_probs - delta_rows[..., None])).astype(jnp.bfloat16)
        grad_query = (
            grad_query
            + jnp.einsum("skgpt,stkd->skgpd", grad_scores, keys, preferred_element_type=jnp.float32)
            * inv_sqrt
        )
        grad_keys = (
            jnp.einsum(
                "skgpt,spkgd->stkd", grad_scores, queries, preferred_element_type=jnp.float32
            )
            * inv_sqrt
        )
        paired = jnp.stack([grad_keys, grad_values], axis=2)
        paired = paired.reshape(seq_count, key_block, piece_len, 2 * kv_heads * head_dim)
        paired = jnp.transpose(paired, (1, 0, 2, 3)).reshape(
            key_block * row_count, 2 * kv_heads * head_dim
        )
        terms = lax.dynamic_update_slice_in_dim(terms, paired, block * (key_block * row_count), 0)
        return (grad_query, terms)

    start = (
        jnp.zeros(grad_heads.shape, jnp.float32),
        jnp.zeros((pieces * row_count, 2 * kv_heads * head_dim), jnp.float32),
    )
    return lax.fori_loop(0, piece // key_block + 1, step, start)


def exchange(value, axis, mask):
    size = lax.axis_size(axis)
    return lax.ppermute(value, axis, [(i, i ^ mask) for i in range(size)])


def gather_blocks(shard):
    half = lax.axis_size("gx") // 2
    near = jnp.concatenate(
        [shard] + [exchange(shard, "gx", 2 * k) for k in range(1, half)], axis=0
    )
    return (near, exchange(near, "gx", 1))


def dot_nn(lhs, rhs):
    return lax.dot_general(lhs, rhs, (((1,), (0,)), ((), ())), preferred_element_type=F32)


def dot_nt(lhs, rhs):
    return lax.dot_general(lhs, rhs, (((1,), (1,)), ((), ())), preferred_element_type=F32)


def dot_tn(lhs, rhs):
    return lax.dot_general(lhs, rhs, (((0,), (0,)), ((), ())), preferred_element_type=F32)


def in_features(pair, weights):
    return dot_nn(pair[0], weights[0]) + dot_nn(pair[1], weights[1])


def reduce_heads(lhs, weights):
    rows = lhs.shape[0] // 2
    width = weights[0].shape[0]
    away = jnp.concatenate([dot_nt(lhs[rows:], w).astype(BF16) for w in weights], axis=1)
    got = exchange(away, "gy", 1)
    own = [
        (dot_nt(lhs[:rows], w) + got[:, i * width : (i + 1) * width].astype(F32)).astype(BF16)
        for i, w in enumerate(weights)
    ]
    own = jnp.concatenate(own, axis=1)
    got = exchange(own, "gy", 2)
    total = (own.astype(F32) + got.astype(F32)).astype(BF16)
    other = exchange(total, "gy", 1)
    return tuple(
        jnp.concatenate(
            [total[:, i * width : (i + 1) * width], other[:, i * width : (i + 1) * width]], axis=0
        ).astype(F32)
        for i in range(2)
    )


def scatter_grad(pair, cols):
    half = lax.axis_size("gx") // 2
    got = exchange(dot_tn(pair[1], cols).astype(BF16), "gx", 1)
    near = dot_tn(pair[0], cols) + got.astype(F32)
    block = near.shape[0] // half
    low = near.astype(BF16)
    total = near[:block]
    for k in range(1, half):
        total = total + exchange(low[k * block : (k + 1) * block], "gx", 2 * k).astype(F32)
    return total


def norm_forward(hidden, gain):
    width = hidden[0].shape[1] * 2
    mean = sum(jnp.sum(h * h, axis=-1, keepdims=True) for h in hidden) / width
    inv_rms = lax.rsqrt(mean + norm_eps)
    normed = tuple((h * inv_rms * g).astype(BF16) for h, g in zip(hidden, gain))
    return (normed, inv_rms)


def norm_backward(grad_normed, hidden, inv_rms, gain):
    width = hidden[0].shape[1] * 2
    unit = [h * inv_rms for h in hidden]
    grad_unit = [d * g for d, g in zip(grad_normed, gain)]
    mean = sum(jnp.sum(d * u, axis=-1, keepdims=True) for d, u in zip(grad_unit, unit)) / width
    grad_hidden = tuple(inv_rms * (d - u * mean) for d, u in zip(grad_unit, unit))
    grad_gain = tuple(jnp.sum(d * u, axis=0) for d, u in zip(grad_normed, unit))
    return (grad_hidden, grad_gain)


def flip_if(bit, value, axis):
    return jnp.where(bit == 1, jnp.flip(value, axis), value)


def to_relative(value, me, core):
    n = lax.axis_size("gx")
    rows, width = value.shape
    bits = n.bit_length() - 1
    shape = (2, rows // 2) + (2,) * bits + (width // n,)
    value = value.reshape(shape)
    value = flip_if(core, value, 0)
    for b in range(bits):
        value = flip_if((me >> (bits - 1 - b)) & 1, value, 2 + b)
    value = value.reshape(rows, n // 2, 2, width // n)
    return tuple(value[:, :, i].reshape(rows, width // 2) for i in range(2))


def from_relative(pair, me, core):
    n = lax.axis_size("gx")
    rows, width = pair[0].shape[0], pair[0].shape[1] * 2
    bits = n.bit_length() - 1
    parts = [h.reshape(rows, n // 2, 1, width // n) for h in pair]
    value = jnp.concatenate(parts, axis=2)
    value = value.reshape((2, rows // 2) + (2,) * bits + (width // n,))
    value = flip_if(core, value, 0)
    for b in range(bits):
        value = flip_if((me >> (bits - 1 - b)) & 1, value, 2 + b)
    return value.reshape(rows, width)


def per_device(
    inputs,
    gain_attn,
    w_query,
    w_key,
    value_projection,
    w_out,
    gain_ffn,
    w_gate,
    w_up,
    w_down,
    cotangent,
):
    pieces = lax.axis_size("gx")
    piece = lax.axis_index("gx")
    core = lax.axis_index("gy") & 1
    row_count = inputs.shape[0]
    seq_count = row_count // P_SIZE
    kv_heads = w_key.shape[2] // HEAD_SIZE
    query_groups = QUERY_HEADS // KEY_VALUE_HEADS
    q_width = w_query.shape[2]
    k_width = w_key.shape[2]
    ff = w_gate.shape[2]
    key_block = min(pieces, max(1, 512 // P_SIZE))
    positions = (piece * P_SIZE + jnp.arange(row_count, dtype=jnp.int32) % P_SIZE).astype(F32)
    cosine_table, sine_table = rope_tables(positions, HEAD_SIZE)

    gains = jnp.concatenate([gain_attn, gain_ffn], axis=0)
    half = pieces // 2
    near = jnp.concatenate([gains] + [exchange(gains, "gx", 2 * k) for k in range(1, half)], axis=1)
    gains = (near.astype(F32), exchange(near, "gx", 1).astype(F32))

    def gain_of(row):
        return tuple(g[row : row + 1] for g in gains)

    layer_weights = []
    for layer in range(DECODER_LAYERS):
        layer_weights.append(
            (
                gather_blocks(
                    jnp.concatenate([w_query[layer], w_key[layer], value_projection[layer]], axis=1)
                ),
                gather_blocks(w_out[layer].T),
                gather_blocks(jnp.concatenate([w_gate[layer], w_up[layer]], axis=1)),
                gather_blocks(w_down[layer].T),
            )
        )

    hidden = to_relative(inputs.astype(F32), piece, core)
    records = []
    for layer in range(DECODER_LAYERS):
        qkv_mat, out_mat, ffn_mat, down_mat = layer_weights[layer]
        normed, inv_attn = norm_forward(hidden, gain_of(layer))
        qkv = in_features(normed, qkv_mat)
        query_lin = qkv[:, :q_width]
        key_linear = qkv[:, q_width : q_width + k_width]
        value_reduced = qkv[:, q_width + k_width :].astype(BF16)
        query_rotated = apply_rotary(
            query_lin.reshape(row_count, kv_heads * query_groups, HEAD_SIZE),
            cosine_table,
            sine_table,
        ).astype(BF16)
        key_rotated = apply_rotary(
            key_linear.reshape(row_count, kv_heads, HEAD_SIZE), cosine_table, sine_table
        ).astype(BF16)
        kv_local = jnp.concatenate([key_rotated.reshape(row_count, k_width), value_reduced], axis=1)
        kv_all = lax.all_gather(kv_local, "gx", axis=0, tiled=True)
        queries = query_rotated.reshape(seq_count, P_SIZE, kv_heads, query_groups, HEAD_SIZE)
        attended, log_total = attend_forward(queries, kv_all, piece, key_block)
        mixed = jnp.transpose(attended, (0, 3, 1, 2, 4)).reshape(row_count, q_width).astype(BF16)
        branch = reduce_heads(mixed, out_mat)
        middle = tuple(h + b for h, b in zip(hidden, branch))
        normed_ffn, inv_ffn = norm_forward(middle, gain_of(DECODER_LAYERS + layer))
        gate_up = in_features(normed_ffn, ffn_mat)
        gate, upward = gate_up[:, :ff], gate_up[:, ff:]
        inner = (jax.nn.silu(gate) * upward).astype(BF16)
        branch = reduce_heads(inner, down_mat)
        records.append(
            (
                hidden,
                normed,
                inv_attn,
                queries,
                kv_all,
                attended,
                log_total,
                mixed,
                middle,
                inv_ffn,
                normed_ffn,
                gate,
                upward,
                inner,
            )
        )
        hidden = tuple(m + b for m, b in zip(middle, branch))
    result = from_relative(hidden, piece, core)

    grad_hidden = to_relative(cotangent, piece, core)
    layer_grads = []
    gain_grads = {}
    for layer in reversed(range(DECODER_LAYERS)):
        (
            hidden,
            normed,
            inv_attn,
            queries,
            kv_all,
            attended,
            log_total,
            mixed,
            middle,
            inv_ffn,
            normed_ffn,
            gate,
            upward,
            inner,
        ) = records[layer]
        qkv_mat, out_mat, ffn_mat, down_mat = layer_weights[layer]
        grad_low = tuple(g.astype(BF16) for g in grad_hidden)
        grad_down = scatter_grad(grad_low, inner)
        grad_inner = in_features(grad_low, down_mat)
        sigmoid_gate = jax.nn.sigmoid(gate)
        grad_gate_low = (
            grad_inner * upward * sigmoid_gate * (1.0 + gate * (1.0 - sigmoid_gate))
        ).astype(BF16)
        grad_up_low = (grad_inner * gate * sigmoid_gate).astype(BF16)
        grad_ffn_low = jnp.concatenate([grad_gate_low, grad_up_low], axis=1)
        grad_ffn = scatter_grad(normed_ffn, grad_ffn_low)
        grad_middle_norm, gain_grads[DECODER_LAYERS + layer] = norm_backward(
            reduce_heads(grad_ffn_low, ffn_mat),
            middle,
            inv_ffn,
            gain_of(DECODER_LAYERS + layer),
        )
        grad_middle = tuple(g + d for g, d in zip(grad_hidden, grad_middle_norm))
        grad_low = tuple(g.astype(BF16) for g in grad_middle)
        grad_out = scatter_grad(grad_low, mixed)
        grad_mixed = in_features(grad_low, out_mat).astype(BF16)
        grad_heads = jnp.transpose(
            grad_mixed.reshape(seq_count, P_SIZE, kv_heads, query_groups, HEAD_SIZE),
            (0, 2, 3, 1, 4),
        )
        delta_rows = jnp.sum(grad_heads.astype(F32) * attended, axis=-1)
        grad_queries, kv_terms = attend_backward(
            queries, kv_all, piece, key_block, log_total, grad_heads, delta_rows, pieces
        )
        kv_grad = lax.psum_scatter(
            kv_terms.astype(BF16), "gx", scatter_dimension=0, tiled=True
        ).astype(F32).reshape(row_count, 2, kv_heads, HEAD_SIZE)
        grad_key_low = (
            rotate_back(kv_grad[:, 0], cosine_table, sine_table)
            .reshape(row_count, k_width)
            .astype(BF16)
        )
        grad_value_low = kv_grad[:, 1].reshape(row_count, k_width).astype(BF16)
        grad_query_rows = jnp.transpose(grad_queries, (0, 3, 1, 2, 4)).reshape(
            row_count, kv_heads * query_groups, HEAD_SIZE
        )
        grad_query_low = (
            rotate_back(grad_query_rows, cosine_table, sine_table)
            .reshape(row_count, q_width)
            .astype(BF16)
        )
        grad_qkv_low = jnp.concatenate([grad_query_low, grad_key_low, grad_value_low], axis=1)
        grad_qkv = scatter_grad(normed, grad_qkv_low)
        grad_in_norm, gain_grads[layer] = norm_backward(
            reduce_heads(grad_qkv_low, qkv_mat), hidden, inv_attn, gain_of(layer)
        )
        grad_hidden = tuple(g + d for g, d in zip(grad_middle, grad_in_norm))
        layer_grads.append((grad_qkv, grad_out, grad_ffn, grad_down))
    layer_grads = layer_grads[::-1]
    gain_near, gain_far = [
        jnp.stack([gain_grads[row][side] for row in range(2 * DECODER_LAYERS)]) for side in range(2)
    ]
    near = gain_near + exchange(gain_far, "gx", 1)
    block = near.shape[1] // half
    gain_total = near[:, :block]
    for k in range(1, half):
        gain_total = gain_total + exchange(near[:, k * block : (k + 1) * block], "gx", 2 * k)
    qkv, out, ffn, down = [jnp.stack([g[i] for g in layer_grads]) for i in range(4)]
    return (
        result,
        from_relative(grad_hidden, piece, core),
        gain_total[:DECODER_LAYERS],
        qkv[:, :, :q_width],
        qkv[:, :, q_width : q_width + k_width],
        qkv[:, :, q_width + k_width :],
        jnp.swapaxes(out, 1, 2),
        gain_total[DECODER_LAYERS:],
        ffn[:, :, :ff],
        ffn[:, :, ff:],
        jnp.swapaxes(down, 1, 2),
    )


def solution(mesh):
    return jax.shard_map(
        per_device,
        mesh=mesh,
        in_specs=(
            P("gx", None),
            P(None, "gx"),
            P(None, "gx", "gy"),
            P(None, "gx", "gy"),
            P(None, "gx", "gy"),
            P(None, "gy", "gx"),
            P(None, "gx"),
            P(None, "gx", "gy"),
            P(None, "gx", "gy"),
            P(None, "gy", "gx"),
            P("gx", None),
        ),
        out_specs=(
            P("gx", None),
            P("gx", None),
            P(None, "gx"),
            P(None, "gx", "gy"),
            P(None, "gx", "gy"),
            P(None, "gx", "gy"),
            P(None, "gy", "gx"),
            P(None, "gx"),
            P(None, "gx", "gy"),
            P(None, "gx", "gy"),
            P(None, "gy", "gx"),
        ),
        check_vma=False,
    )
```

```python
import functools

import jax
import jax.numpy as jnp
from jax import lax
from jax.experimental import pallas as pl
from jax.experimental.pallas import tpu as pltpu
from jax.sharding import PartitionSpec as P

QUERY_HEADS = 16
KEY_VALUE_HEADS = 8
HEAD_SIZE = 96
DECODER_LAYERS = 2
P_SIZE = 128

norm_eps = 1e-05
rope_base = 100000.0
big_negative = -1e30
F32 = jnp.float32
BF16 = jnp.bfloat16
MESH = pl.DeviceIdType.MESH


GROUPS = 5
CHUNKS = 4
QROWS = 256
UNIT = 4 * HEAD_SIZE
inv_sqrt = HEAD_SIZE**-0.5
AHEAD = 3


def dot_nn(lhs, rhs):
    return lax.dot_general(lhs, rhs, (((1,), (0,)), ((), ())), preferred_element_type=F32)


def dot_nt(lhs, rhs):
    return lax.dot_general(lhs, rhs, (((1,), (1,)), ((), ())), preferred_element_type=F32)


def dot_tn(lhs, rhs):
    return lax.dot_general(lhs, rhs, (((0,), (0,)), ((), ())), preferred_element_type=F32)


def remote(src, dst, send_sem, recv_sem, **device):
    return pltpu.make_async_remote_copy(
        src_ref=src,
        dst_ref=dst,
        send_sem=send_sem,
        recv_sem=recv_sem,
        device_id=device,
        device_id_type=MESH,
    )


class Place:
    def __init__(self, n):
        self.n = n
        self.half = n // 2
        self.me = lax.axis_index("gx")
        self.z = self.me // 2
        self.x = self.me % 2
        self.across = self.me + 1 - 2 * self.x
        gy = lax.axis_index("gy")
        self.core = gy % 2
        self.twin = gy + 1 - 2 * self.core
        self.far = (gy + 2) % 4

    def column(self, k):
        return ((self.z + k) % self.half) * 2 + self.x

    def column_back(self, k):
        return ((self.z + self.half - k) % self.half) * 2 + self.x

    def greet(self):
        barrier = pltpu.get_barrier_semaphore()
        for k in range(1, self.n):
            peer = (self.me + k) % self.n
            pl.semaphore_signal(barrier, inc=1, device_id={"gx": peer}, device_id_type=MESH)
        for peer in (self.twin, self.far):
            pl.semaphore_signal(barrier, inc=1, device_id={"gy": peer}, device_id_type=MESH)
        pl.semaphore_wait(barrier, self.n + 1)


class Gather:
    def __init__(self, at, shards, full, order, sems):
        self.at, self.shards, self.full, self.order = at, shards, full, order
        self.z_send, self.z_recv, self.x_send, self.x_recv, self.own = sems
        self.pumped = 0
        self.done = 0
        self.started = []

    def z_copy(self, g, k):
        layer, kind = self.order[g]
        i = g * (self.at.half - 1) + k - 1
        return remote(
            self.shards[kind].at[layer],
            self.full[kind].at[layer, self.at.me],
            self.z_send.at[i],
            self.z_recv.at[i],
            gx=self.at.column(k),
        )

    def x_copy(self, g, k):
        layer, kind = self.order[g]
        i = g * self.at.half + k
        block = self.at.column_back(k) if k else self.at.me
        target = self.full[kind].at[layer, block]
        return remote(
            target if k else self.shards[kind].at[layer],
            target,
            self.x_send.at[i],
            self.x_recv.at[i],
            gx=self.at.across,
        )

    def own_copy(self, g):
        layer, kind = self.order[g]
        return pltpu.make_async_copy(
            self.shards[kind].at[layer], self.full[kind].at[layer, self.at.me], self.own.at[g]
        )

    def begin(self, g):
        if g < len(self.order):
            for k in range(1, self.at.half):
                self.z_copy(g, k).start()
            self.x_copy(g, 0).start()
            self.own_copy(g).start()

    def open(self):
        for g in range(AHEAD):
            self.begin(g)

    def pump(self):
        g = self.pumped
        if g < len(self.order):
            self.pumped += 1
            for k in range(1, self.at.half):
                self.z_copy(g, k).wait_recv()
                self.x_copy(g, k).start()
            self.begin(g + AHEAD)

    def need(self, g):
        while self.pumped < min(g + 2, len(self.order)):
            self.pump()
        while self.done <= g:
            for k in range(self.at.half):
                self.x_copy(self.done, k).wait_recv()
            self.own_copy(self.done).wait()
            self.done += 1

    def close(self):
        for g in range(len(self.order)):
            for k in range(1, self.at.half):
                self.z_copy(g, k).wait_send()
            for k in range(self.at.half):
                self.x_copy(g, k).wait_send()


def all_to_all(at, src, dst, send, recv):
    copies = [
        remote(
            src.at[(at.me + k) % at.n],
            dst.at[at.me],
            send.at[k - 1],
            recv.at[k - 1],
            gx=(at.me + k) % at.n,
        )
        for k in range(1, at.n)
    ]
    own = pltpu.make_async_copy(src.at[at.me], dst.at[at.me], send.at[at.n - 1])
    for copy in copies:
        copy.start()
    own.start()
    return copies, own


def finish_all(copies):
    remotes, own = copies
    own.wait()
    for copy in remotes:
        copy.wait()


class HeadSum:
    def __init__(self, at, bufs, sems):
        self.at = at
        self.away, self.got1, self.mine, self.got2, self.got3 = bufs
        self.sems = sems
        self.calls = 0

    def __call__(self, row_count, product, put, between=lambda: None):
        at, slot = self.at, self.calls % 2
        self.calls += 1
        rows = row_count // 2
        own = pl.ds(pl.multiple_of(at.core * rows, rows), rows)
        other = pl.ds(pl.multiple_of((1 - at.core) * rows, rows), rows)

        def copy(phase, i):
            src, dst, device = (
                (self.away.at[i], self.got1.at[i], {"gy": at.twin}),
                (self.mine.at[i], self.got2.at[slot, i], {"gy": at.far}),
                (self.away.at[i], self.got3.at[i], {"gy": at.twin}),
            )[phase]
            k = (slot * 3 + phase) * CHUNKS + i
            return remote(src, dst, self.sems[0].at[k], self.sems[1].at[k], **device)

        for i in range(CHUNKS):
            self.away[i] = product(other, i).astype(BF16)
            copy(0, i).start()
        for i in range(CHUNKS):
            part = product(own, i)
            copy(0, i).wait()
            self.mine[i] = (part + self.got1[i].astype(F32)).astype(BF16)
            copy(1, i).start()
        between()
        for i in range(CHUNKS):
            copy(1, i).wait()
            self.away[i] = (self.mine[i].astype(F32) + self.got2[slot, i].astype(F32)).astype(BF16)
            copy(2, i).start()
            put(own, i, self.away[i].astype(F32))
        for i in range(CHUNKS):
            copy(2, i).wait()
            put(other, i, self.got3[i].astype(F32))


def feature_chunk(ref, i, n, cols):
    per = n // CHUNKS
    value = ref[i * per : (i + 1) * per, :, cols]
    return value.reshape(value.shape[0] * value.shape[1], value.shape[2])


def rows_loop(rows, step, body):
    def once(r, carry):
        body(pl.ds(pl.multiple_of(r * step, step), step))
        return carry

    lax.fori_loop(0, rows // step, once, 0)


def norm_rows(src, dst, gain):
    def body(here):
        value = src[here, :]
        mean = jnp.mean(value * value, axis=-1, keepdims=True)
        dst[here, :] = (value * lax.rsqrt(mean + norm_eps) * gain).astype(BF16)

    rows_loop(src.shape[0], 64, body)


def turn(value, tables, sign):
    cosine, low, high = tables
    width = value.shape[1]
    half = HEAD_SIZE // 2
    left = pltpu.roll(value, width - half, axis=1)
    right = pltpu.roll(value, half, axis=1)
    return value * cosine + sign * (left * low + right * high)


def split_unit(unit, q_ref, k_ref, v_ref):
    size = HEAD_SIZE
    for b in range(unit.shape[0]):
        value = unit[b]
        here = slice(b * P_SIZE, (b + 1) * P_SIZE)
        q_ref[0, here, :] = value[:, :size]
        q_ref[1, here, :] = value[:, size : 2 * size]
        k_ref[here, :] = value[:, 2 * size : 3 * size]
        v_ref[here, :] = value[:, 3 * size :]


def probabilities(query, keys, first):
    scores = dot_nt(keys, query) * inv_sqrt
    key = lax.broadcasted_iota(jnp.int32, scores.shape, 0)
    row = lax.broadcasted_iota(jnp.int32, scores.shape, 1) + first
    scores = jnp.where(key <= row, scores, big_negative)
    expo = jnp.exp(scores - jnp.max(scores, axis=0, keepdims=True))
    return expo * (1.0 / jnp.sum(expo, axis=0, keepdims=True))


def forward_kernel(n, row_count, *refs):
    refs = list(refs)

    def take(count):
        out = refs[:count]
        del refs[:count]
        return out if count > 1 else out[0]

    inputs, gains_in, cosine, low, high = take(5)
    shards = take(GROUPS)
    result, hidden_out, middle_out, gate_out, up_out, unit_out, mixed_out, gain_out = take(8)
    full = take(GROUPS)
    cur, normed, gain_all, qkv_lin, unit_send, unit, q_ref, k_ref, v_ref = take(9)
    attended, mix_back, mixed, gate, up, inner = take(6)
    weights = take(GROUPS)
    bufs = take(5)
    z_send, z_recv, x_send, x_recv, own_sem = take(5)
    a2a_send, a2a_recv, sum_send, sum_recv, gain_send, gain_recv, load_sem, save_sem = take(8)

    at = Place(n)
    units = n
    kv_heads = units * P_SIZE // row_count
    width = cur.shape[1]
    chunk = width // CHUNKS
    order = [(layer, kind) for layer in range(DECODER_LAYERS) for kind in range(GROUPS)]
    ag = Gather(at, shards, full, order, (z_send, z_recv, x_send, x_recv, own_sem))
    head_sum = HeadSum(at, bufs, (sum_send, sum_recv))

    at.greet()
    gain_copies = [
        remote(
            gains_in,
            gain_all.at[at.me],
            gain_send.at[k - 1],
            gain_recv.at[k - 1],
            gx=(at.me + k) % n,
        )
        for k in range(1, n)
    ]
    for copy in gain_copies:
        copy.start()
    own_gain = pltpu.make_async_copy(gains_in, gain_all.at[at.me], gain_send.at[n - 1])
    own_gain.start()
    ag.open()

    def widen(here):
        cur[here, :] = inputs[here, :].astype(F32)

    rows_loop(row_count, 64, widen)
    own_gain.wait()
    for copy in gain_copies:
        copy.wait()
    blk = width // n
    for b in range(n):
        gain_out[:, b * blk : (b + 1) * blk] = gain_all[b][:, :blk]

    saves = []

    def save(src, dst, i, later=True):
        copy = pltpu.make_async_copy(src, dst, save_sem.at[i])
        copy.start()
        if later:
            saves.append(copy)
        return copy

    def load(g):
        ag.need(g)
        layer, kind = order[g]
        copy = pltpu.make_async_copy(full[kind].at[layer], weights[kind], load_sem.at[kind])
        copy.start()
        return copy

    def product_of(lhs, ref):
        return lambda rows, i: dot_nt(lhs[rows, :], feature_chunk(ref, i, n, slice(None)))

    def add_to_cur(here, i, value):
        cols = slice(i * chunk, (i + 1) * chunk)
        cur[here, cols] = cur[here, cols] + value

    pending = save(cur, hidden_out.at[0], 15, False)
    for layer in range(DECODER_LAYERS):
        base = layer * GROUPS
        norm_rows(cur, normed, gain_out[layer : layer + 1, :])
        load(base).wait()
        for u in range(kv_heads):
            w = weights[0][:, :, u * UNIT : (u + 1) * UNIT].reshape(width, UNIT)
            qkv_lin[...] = dot_nn(normed[...], w)
            for s in range(row_count // P_SIZE):
                value = qkv_lin[s * P_SIZE : (s + 1) * P_SIZE, :]
                value = turn(value, (cosine[...], low[...], high[...]), 1.0)
                unit_send[s * kv_heads + u] = value.astype(BF16)
        copies = all_to_all(
            at, unit_send, unit.at[layer], a2a_send.at[2 * layer], a2a_recv.at[2 * layer]
        )
        ag.pump()
        finish_all(copies)
        save(unit.at[layer], unit_out.at[layer], 5 * layer)
        split_unit(unit.at[layer], q_ref, k_ref, v_ref)
        v_turned = v_ref[...].T
        for qb in range(n * P_SIZE // QROWS):
            here = slice(qb * QROWS, (qb + 1) * QROWS)
            keys = (qb + 1) * QROWS
            outs = []
            for h in range(2):
                probs = probabilities(q_ref[h, here, :], k_ref[:keys, :], qb * QROWS)
                outs.append(dot_nn(v_turned[:, :keys], probs.astype(BF16)))
            both = jnp.concatenate(outs, axis=0).T.astype(BF16)
            for i in range(QROWS // P_SIZE):
                attended[layer, qb * (QROWS // P_SIZE) + i] = both[i * P_SIZE : (i + 1) * P_SIZE]
        copies = all_to_all(
            at,
            attended.at[layer],
            mix_back.at[layer],
            a2a_send.at[2 * layer + 1],
            a2a_recv.at[2 * layer + 1],
        )
        out_load = load(base + 1)
        finish_all(copies)
        for s in range(row_count // P_SIZE):
            parts = [mix_back[layer, s * kv_heads + u] for u in range(kv_heads)]
            mixed[s * P_SIZE : (s + 1) * P_SIZE, :] = jnp.concatenate(parts, axis=1)
        out_load.wait()
        pending.wait()
        mixed_save = save(mixed, mixed_out.at[layer], 5 * layer + 4, False)
        head_sum(row_count, product_of(mixed, weights[1]), add_to_cur, ag.pump)
        middle_save = save(cur, middle_out.at[layer], 5 * layer + 2, False)
        norm_rows(cur, normed, gain_out[DECODER_LAYERS + layer : DECODER_LAYERS + layer + 1, :])
        loads = [load(base + 2), load(base + 3)]
        for copy in loads:
            copy.wait()

        def tile(t, carry):
            cols = pl.ds(pl.multiple_of(t * 256, 256), 256)
            g = dot_nn(normed[...], weights[2][:, :, cols].reshape(width, 256))
            v = dot_nn(normed[...], weights[3][:, :, cols].reshape(width, 256))
            gate[:, cols] = g
            up[:, cols] = v
            inner[:, cols] = (g * (1.0 / (1.0 + jnp.exp(-g))) * v).astype(BF16)
            return carry

        lax.fori_loop(0, gate.shape[1] // 256, tile, 0)
        gate_saves = [
            pltpu.make_async_copy(gate, gate_out.at[layer], save_sem.at[10 + 2 * layer]),
            pltpu.make_async_copy(up, up_out.at[layer], save_sem.at[11 + 2 * layer]),
        ]
        for copy in gate_saves:
            copy.start()
        load(base + 4).wait()
        middle_save.wait()
        mixed_save.wait()
        head_sum(row_count, product_of(inner, weights[4]), add_to_cur, ag.pump)
        for copy in gate_saves:
            copy.wait()
        if layer < DECODER_LAYERS - 1:
            pending = save(cur, hidden_out.at[layer + 1], 5 * layer + 3, False)
    save(cur, result, 14)
    for copy in saves:
        copy.wait()
    ag.close()


def forward(n, inputs, gains, tables, shards):
    row_count, width = inputs.shape
    half = n // 2
    groups = DECODER_LAYERS * GROUPS
    ff = shards[2].shape[2]
    q_cols = shards[1].shape[2]
    any_space = pl.BlockSpec(memory_space=pl.ANY)
    vmem = pl.BlockSpec(memory_space=pltpu.VMEM)
    blk = width // n
    layers = DECODER_LAYERS
    out_shape = (
        [jax.ShapeDtypeStruct((row_count, width), F32)]
        + [jax.ShapeDtypeStruct((layers, row_count, width), F32)] * 2
        + [jax.ShapeDtypeStruct((layers, row_count, ff), F32)] * 2
        + [
            jax.ShapeDtypeStruct((layers, n, P_SIZE, UNIT), BF16),
            jax.ShapeDtypeStruct((layers, row_count, q_cols), BF16),
            jax.ShapeDtypeStruct((8, width), F32),
        ]
        + [jax.ShapeDtypeStruct((layers, n, blk, s.shape[2]), BF16) for s in shards]
    )
    seq = n * P_SIZE
    piece = (CHUNKS, row_count // 2, width // CHUNKS)
    scratch = (
        [
            pltpu.VMEM((row_count, width), F32),
            pltpu.VMEM((row_count, width), BF16),
            pltpu.VMEM((n,) + gains.shape, F32),
            pltpu.VMEM((row_count, UNIT), F32),
            pltpu.VMEM((n, P_SIZE, UNIT), BF16),
            pltpu.VMEM((layers, n, P_SIZE, UNIT), BF16),
            pltpu.VMEM((2, seq, HEAD_SIZE), BF16),
            pltpu.VMEM((seq, HEAD_SIZE), BF16),
            pltpu.VMEM((seq, HEAD_SIZE), BF16),
            pltpu.VMEM((layers, n, P_SIZE, UNIT // 2), BF16),
            pltpu.VMEM((layers, n, P_SIZE, UNIT // 2), BF16),
            pltpu.VMEM((row_count, q_cols), BF16),
            pltpu.VMEM((row_count, ff), F32),
            pltpu.VMEM((row_count, ff), F32),
            pltpu.VMEM((row_count, ff), BF16),
        ]
        + [pltpu.VMEM((n, blk, s.shape[2]), BF16) for s in shards]
        + [
            pltpu.VMEM(piece, BF16),
            pltpu.VMEM(piece, BF16),
            pltpu.VMEM(piece, BF16),
            pltpu.VMEM((2,) + piece, BF16),
            pltpu.VMEM(piece, BF16),
        ]
        + [
            pltpu.SemaphoreType.DMA((groups * (half - 1),)),
            pltpu.SemaphoreType.DMA((groups * (half - 1),)),
            pltpu.SemaphoreType.DMA((groups * half,)),
            pltpu.SemaphoreType.DMA((groups * half,)),
            pltpu.SemaphoreType.DMA((groups,)),
            pltpu.SemaphoreType.DMA((2 * layers, n)),
            pltpu.SemaphoreType.DMA((2 * layers, n)),
            pltpu.SemaphoreType.DMA((6 * CHUNKS,)),
            pltpu.SemaphoreType.DMA((6 * CHUNKS,)),
            pltpu.SemaphoreType.DMA((n,)),
            pltpu.SemaphoreType.DMA((n,)),
            pltpu.SemaphoreType.DMA((GROUPS,)),
            pltpu.SemaphoreType.DMA((16,)),
        ]
    )
    return pl.pallas_call(
        functools.partial(forward_kernel, n, row_count),
        out_shape=out_shape,
        in_specs=[vmem] * (5 + GROUPS),
        out_specs=[any_space] * 7 + [vmem] + [any_space] * GROUPS,
        scratch_shapes=scratch,
        compiler_params=pltpu.CompilerParams(
            collective_id=0, has_side_effects=True, vmem_limit_bytes=60 * 1024 * 1024
        ),
        name="forward_layers",
    )(inputs, gains, *tables, *shards)


class Scatter:
    def __init__(self, at, send, got_x, got_z, outs, stage, sems):
        self.at, self.send, self.got_x, self.got_z = at, send, got_x, got_z
        self.outs, self.stage = outs, stage
        self.x_send, self.x_recv, self.z_send, self.z_recv, self.out_sem = sems[:5]
        self.free_x, self.free_z = sems[5:]
        self.leaving = None

    def tiles(self, kind, body):
        width = self.send[kind].shape[2]
        step = 256 if width % 256 == 0 else 128

        def once(t, carry):
            body(pl.ds(pl.multiple_of(t * step, step), step))
            return carry

        lax.fori_loop(0, width // step, once, 0)

    def x_copy(self, layer, kind):
        i = layer * GROUPS + kind
        return remote(
            self.send[kind],
            self.got_x[kind],
            self.x_send.at[i],
            self.x_recv.at[i],
            gx=self.at.across,
        )

    def z_copy(self, layer, kind, k):
        i = (layer * GROUPS + kind) * (self.at.half - 1) + k - 1
        return remote(
            self.send[kind].at[(self.at.z + k) % self.at.half],
            self.got_z[kind].at[k - 1],
            self.z_send.at[i],
            self.z_recv.at[i],
            gx=self.at.column(k),
        )

    def product(self, turned, side, cols):
        lhs = turned[side]
        return dot_nn(lhs.reshape(lhs.shape[0] * lhs.shape[1], lhs.shape[2]), cols)

    def first(self, layer, kind, turned, cols_of):
        def body(tile):
            part = self.product(turned, 1 - self.at.x, cols_of(tile))
            block = self.send[kind].shape
            self.send[kind][:, :, tile] = part.reshape(block[0], block[1], -1).astype(BF16)

        self.tiles(kind, body)
        if layer < DECODER_LAYERS - 1:
            pl.semaphore_wait(self.free_x.at[kind], 1)
        self.x_copy(layer, kind).start()

    def second(self, layer, kind, turned, cols_of):
        self.x_copy(layer, kind).wait()

        def body(tile):
            part = self.product(turned, self.at.x, cols_of(tile))
            block = self.send[kind].shape
            part = part.reshape(block[0], block[1], -1)
            self.send[kind][:, :, tile] = (
                part + self.got_x[kind][:, :, tile].astype(F32)
            ).astype(BF16)

        self.tiles(kind, body)
        if layer > 0:
            pl.semaphore_signal(
                self.free_x.at[kind], inc=1, device_id={"gx": self.at.across}, device_id_type=MESH
            )
        for k in range(1, self.at.half):
            if layer < DECODER_LAYERS - 1:
                pl.semaphore_wait(self.free_z.at[kind * (self.at.half - 1) + k - 1], 1)
            self.z_copy(layer, kind, k).start()

    def last(self, layer, kind):
        for k in range(1, self.at.half):
            self.z_copy(layer, kind, k).wait()
        if self.leaving is not None:
            self.leaving.wait()
        width = self.send[kind].shape[2]
        total = self.send[kind][self.at.z].astype(F32)
        for k in range(1, self.at.half):
            total = total + self.got_z[kind][k - 1].astype(F32)
        self.stage[:, :width] = total
        if layer > 0:
            for k in range(1, self.at.half):
                pl.semaphore_signal(
                    self.free_z.at[kind * (self.at.half - 1) + k - 1],
                    inc=1,
                    device_id={"gx": self.at.column_back(k)},
                    device_id_type=MESH,
                )
        self.leaving = pltpu.make_async_copy(
            self.stage.at[:, :width], self.outs[kind].at[layer], self.out_sem
        )
        self.leaving.start()


def turn_rows(value_of, dst, row_count, n):
    def once(r, carry):
        here = pl.ds(pl.multiple_of(r * 128, 128), 128)
        turned = value_of(here).T
        blk = turned.shape[0] // n
        for b in range(n):
            dst[b % 2, b // 2, :, here] = turned[b * blk : (b + 1) * blk]
        return carry

    lax.fori_loop(0, row_count // 128, once, 0)


def backward_kernel(n, row_count, *refs):
    refs = list(refs)

    def take(count):
        out = refs[:count]
        del refs[:count]
        return out if count > 1 else out[0]

    cotangent, hidden_in, middle_in, gate_in, up_in, unit_in, mixed_in = take(7)
    gain_all, cosine, low_sine, high_sine = take(4)
    full = take(GROUPS)
    grad_out, gain_out = take(2)
    outs = take(GROUPS)
    grad, kept, arrived, gate, up, inner, grad_ffn, low = take(8)
    turned_grad, turned_unit, mat_a, mat_b, mat_c = take(5)
    unit, q_ref, k_ref, v_ref, do_send, do_unit, dq_ref, dk_ref, dv_ref = take(9)
    home, qkv_grad, mixed, gain_sum, gain_send, gain_got = take(6)
    unit_grad = unit
    bufs = take(5)
    send = take(GROUPS)
    got_x = take(GROUPS)
    got_z = take(GROUPS)
    stage = take(1)
    x_send, x_recv, z_send, z_recv, out_sem, free_x, free_z = take(7)
    a2a_send, a2a_recv, sum_send, sum_recv, gain_s, gain_r, load_sem = take(7)

    at = Place(n)
    kv_heads = n * P_SIZE // row_count
    width = grad.shape[1]
    ff = gate.shape[1]
    chunk = width // CHUNKS
    blk = width // n
    seqs = row_count // P_SIZE
    rs = Scatter(
        at,
        send,
        got_x,
        got_z,
        outs,
        stage,
        (x_send, x_recv, z_send, z_recv, out_sem, free_x, free_z),
    )
    head_sum = HeadSum(at, bufs, (sum_send, sum_recv))
    tables = (cosine[...], low_sine[...], high_sine[...])

    def load(src, dst, i):
        copy = pltpu.make_async_copy(src, dst, load_sem.at[i])
        copy.start()
        return copy

    def narrow(ref, kind):
        return ref.at[:, :, : full[kind].shape[3]]

    def layer_loads(layer):
        return {
            "gate": load(gate_in.at[layer], gate, 0),
            "up": load(up_in.at[layer], up, 1),
            "down_w": load(full[4].at[layer], mat_a, 2),
            "kept": load(middle_in.at[layer], kept, 3),
            "gate_w": load(full[2].at[layer], mat_b, 4),
            "up_w": load(full[3].at[layer], mat_c, 5),
            "mixed": load(mixed_in.at[layer], mixed, 6),
            "unit": load(unit_in.at[layer], unit, 7),
        }

    def put(here, i, value):
        arrived[here, i * chunk : (i + 1) * chunk] = value

    def normed(row):
        gain = gain_all[row : row + 1, :]

        def value_of(here):
            value = kept[here, :]
            mean = jnp.mean(value * value, axis=-1, keepdims=True)
            return (value * lax.rsqrt(mean + norm_eps) * gain).astype(BF16)

        return value_of

    def lowered(here):
        value = grad[here, :].astype(BF16)
        low[here, :] = value
        return value

    def norm_back(row):
        gain = gain_all[row : row + 1, :]

        def body(here):
            value = kept[here, :]
            factor = lax.rsqrt(jnp.mean(value * value, axis=-1, keepdims=True) + norm_eps)
            unit_rows = value * factor
            grad_normed = arrived[here, :]
            grad_unit = grad_normed * gain
            mean = jnp.mean(grad_unit * unit_rows, axis=-1, keepdims=True)
            grad[here, :] = grad[here, :] + factor * (grad_unit - unit_rows * mean)
            terms = (grad_normed * unit_rows).reshape(8, 8, width)
            gain_sum[row] = gain_sum[row] + jnp.sum(terms, axis=0)

        rows_loop(row_count, 64, body)

    start = load(cotangent, grad, 8)
    loads = layer_loads(DECODER_LAYERS - 1)
    gain_sum[...] = jnp.zeros_like(gain_sum)
    at.greet()
    start.wait()
    for layer in reversed(range(DECODER_LAYERS)):
        ffn_row, attn_row = DECODER_LAYERS + layer, layer
        turn_rows(lowered, turned_grad, row_count, n)
        loads["gate"].wait()
        loads["up"].wait()

        def activate(here):
            g = gate[here, :]
            inner[here, :] = (g * (1.0 / (1.0 + jnp.exp(-g))) * up[here, :]).astype(BF16)

        rows_loop(row_count, 64, activate)
        rs.first(layer, 4, turned_grad, lambda t: inner[:, t])
        loads["down_w"].wait()

        def tile(t, carry):
            cols = pl.ds(pl.multiple_of(t * 256, 256), 256)
            upper = pl.ds(pl.multiple_of(ff + t * 256, 256), 256)
            dz = dot_nn(low[...], mat_a[:, :, cols].reshape(width, 256))
            g = gate[:, cols]
            sig = 1.0 / (1.0 + jnp.exp(-g))
            grad_ffn[:, cols] = (dz * up[:, cols] * sig * (1.0 + g * (1.0 - sig))).astype(BF16)
            grad_ffn[:, upper] = (dz * g * sig).astype(BF16)
            return carry

        lax.fori_loop(0, ff // 256, tile, 0)
        qkv_load = load(full[0].at[layer], narrow(mat_a, 0), 2)
        loads["kept"].wait()
        turn_rows(normed(ffn_row), turned_unit, row_count, n)
        gate_cols = lambda t: grad_ffn[:, t]
        up_cols = lambda t: grad_ffn[:, pl.ds(pl.multiple_of(ff + t.start, 128), t.size)]
        rs.first(layer, 2, turned_unit, gate_cols)
        rs.first(layer, 3, turned_unit, up_cols)
        loads["gate_w"].wait()
        loads["up_w"].wait()

        def product(rows, i):
            return dot_nt(
                grad_ffn[rows, :ff], feature_chunk(mat_b, i, n, slice(None))
            ) + dot_nt(grad_ffn[rows, ff:], feature_chunk(mat_c, i, n, slice(None)))

        head_sum(row_count, product, put)
        out_load = load(full[1].at[layer], narrow(mat_b, 1), 4)
        norm_back(ffn_row)
        kept_load = load(hidden_in.at[layer], kept, 3)
        rs.second(layer, 4, turned_grad, lambda t: inner[:, t])
        turn_rows(lowered, turned_grad, row_count, n)
        loads["mixed"].wait()
        rs.first(layer, 1, turned_grad, lambda t: mixed[:, t])
        out_load.wait()
        q_cols = full[1].shape[3]
        for s in range(seqs):
            here = slice(s * P_SIZE, (s + 1) * P_SIZE)
            value = dot_nn(low[here, :], mat_b[:, :, :q_cols].reshape(width, q_cols)).astype(BF16)
            for u in range(kv_heads):
                do_send[s * kv_heads + u] = value[:, u * UNIT // 2 : (u + 1) * UNIT // 2]
        copies = all_to_all(at, do_send, do_unit, a2a_send.at[2 * layer], a2a_recv.at[2 * layer])
        loads["unit"].wait()
        split_unit(unit, q_ref, k_ref, v_ref)
        k_turned = k_ref[...].T
        dk_ref[...] = jnp.zeros_like(dk_ref)
        dv_ref[...] = jnp.zeros_like(dv_ref)
        finish_all(copies)
        per = QROWS // P_SIZE
        for qb in range(n * P_SIZE // QROWS):
            here = slice(qb * QROWS, (qb + 1) * QROWS)
            keys = (qb + 1) * QROWS
            grads = do_unit[qb * per : (qb + 1) * per].reshape(QROWS, UNIT // 2)
            outs_q = []
            for h in range(2):
                query = q_ref[h, here, :]
                probs = probabilities(query, k_ref[:keys, :], qb * QROWS)
                grad_head = grads[:, h * HEAD_SIZE : (h + 1) * HEAD_SIZE]
                grad_probs = dot_nt(v_ref[:keys, :], grad_head)
                delta = jnp.sum(probs * grad_probs, axis=0, keepdims=True)
                grad_scores = (probs * (grad_probs - delta)).astype(BF16)
                dv_ref[:keys, :] += dot_nn(probs.astype(BF16), grad_head)
                dk_ref[:keys, :] += dot_nn(grad_scores, query)
                outs_q.append(dot_nn(k_turned[:, :keys], grad_scores) * inv_sqrt)
            dq_ref[here, :] = jnp.concatenate(outs_q, axis=0).T.astype(BF16)
        for b in range(n):
            here = slice(b * P_SIZE, (b + 1) * P_SIZE)
            unit_grad[b] = jnp.concatenate(
                [
                    dq_ref[here, :],
                    (dk_ref[here, :] * inv_sqrt).astype(BF16),
                    dv_ref[here, :].astype(BF16),
                ],
                axis=1,
            )
        copies = all_to_all(
            at, unit_grad, home, a2a_send.at[2 * layer + 1], a2a_recv.at[2 * layer + 1]
        )
        rs.second(layer, 2, turned_unit, gate_cols)
        finish_all(copies)
        for s in range(seqs):
            for u in range(kv_heads):
                value = home[s * kv_heads + u].astype(F32)
                qkv_grad[s * P_SIZE : (s + 1) * P_SIZE, u * UNIT : (u + 1) * UNIT] = turn(
                    value, tables, -1.0
                ).astype(BF16)
        rs.second(layer, 3, turned_unit, up_cols)
        kept_load.wait()
        turn_rows(normed(attn_row), turned_unit, row_count, n)
        rs.first(layer, 0, turned_unit, lambda t: qkv_grad[:, t])
        rs.last(layer, 4)
        qkv_load.wait()
        qkv_cols = full[0].shape[3]

        def product(rows, i):
            return dot_nt(qkv_grad[rows, :], feature_chunk(mat_a, i, n, slice(0, qkv_cols)))

        head_sum(row_count, product, put)
        norm_back(attn_row)
        rs.second(layer, 1, turned_grad, lambda t: mixed[:, t])
        if layer > 0:
            loads = layer_loads(layer - 1)
        else:
            final = load(grad, grad_out, 8)
            for row in range(2 * DECODER_LAYERS):
                total = jnp.sum(gain_sum[row], axis=0, keepdims=True)
                for b in range(n):
                    gain_send[b, row : row + 1, :blk] = total[:, b * blk : (b + 1) * blk]
            gain_copies = all_to_all(at, gain_send, gain_got, gain_s, gain_r)
        rs.last(layer, 2)
        rs.second(layer, 0, turned_unit, lambda t: qkv_grad[:, t])
        rs.last(layer, 3)
        rs.last(layer, 1)
        if layer == 0:
            finish_all(gain_copies)
            total = gain_got[0]
            for b in range(1, n):
                total = total + gain_got[b]
            gain_out[...] = total
        rs.last(layer, 0)
    rs.leaving.wait()
    final.wait()


def backward(n, cotangent, saved, gain_all, tables, full):
    row_count, width = cotangent.shape
    half = n // 2
    layers = DECODER_LAYERS
    groups = layers * GROUPS
    ff = full[2].shape[3]
    q_cols = full[1].shape[3]
    qkv_cols = full[0].shape[3]
    blk = width // n
    seq = n * P_SIZE
    lanes = -(-blk // 128) * 128
    cols = [f.shape[3] for f in full]
    any_space = pl.BlockSpec(memory_space=pl.ANY)
    vmem = pl.BlockSpec(memory_space=pltpu.VMEM)
    piece = (CHUNKS, row_count // 2, width // CHUNKS)
    rows_f32 = pltpu.VMEM((row_count, width), F32)
    scratch = (
        [
            rows_f32,
            rows_f32,
            rows_f32,
            pltpu.VMEM((row_count, ff), F32),
            pltpu.VMEM((row_count, ff), F32),
            pltpu.VMEM((row_count, ff), BF16),
            pltpu.VMEM((row_count, 2 * ff), BF16),
            pltpu.VMEM((row_count, width), BF16),
            pltpu.VMEM((2, half, blk, row_count), BF16),
            pltpu.VMEM((2, half, blk, row_count), BF16),
        ]
        + [pltpu.VMEM((n, blk, ff), BF16)] * 3
        + [
            pltpu.VMEM((n, P_SIZE, UNIT), BF16),
            pltpu.VMEM((2, seq, HEAD_SIZE), BF16),
            pltpu.VMEM((seq, HEAD_SIZE), BF16),
            pltpu.VMEM((seq, HEAD_SIZE), BF16),
            pltpu.VMEM((n, P_SIZE, UNIT // 2), BF16),
            pltpu.VMEM((n, P_SIZE, UNIT // 2), BF16),
            pltpu.VMEM((seq, UNIT // 2), BF16),
            pltpu.VMEM((seq, HEAD_SIZE), F32),
            pltpu.VMEM((seq, HEAD_SIZE), F32),
            pltpu.VMEM((n, P_SIZE, UNIT), BF16),
            pltpu.VMEM((row_count, qkv_cols), BF16),
            pltpu.VMEM((row_count, q_cols), BF16),
            pltpu.VMEM((8, 8, width), F32),
            pltpu.VMEM((n, 8, lanes), F32),
            pltpu.VMEM((n, 8, lanes), F32),
        ]
        + [
            pltpu.VMEM(piece, BF16),
            pltpu.VMEM(piece, BF16),
            pltpu.VMEM(piece, BF16),
            pltpu.VMEM((2,) + piece, BF16),
            pltpu.VMEM(piece, BF16),
        ]
        + [pltpu.VMEM((half, blk, c), BF16) for c in cols]
        + [pltpu.VMEM((half, blk, c), BF16) for c in cols]
        + [pltpu.VMEM((half - 1, blk, c), BF16) for c in cols]
        + [pltpu.VMEM((blk, max(cols)), F32)]
        + [
            pltpu.SemaphoreType.DMA((groups,)),
            pltpu.SemaphoreType.DMA((groups,)),
            pltpu.SemaphoreType.DMA((groups * (half - 1),)),
            pltpu.SemaphoreType.DMA((groups * (half - 1),)),
            pltpu.SemaphoreType.DMA,
            pltpu.SemaphoreType.REGULAR((GROUPS,)),
            pltpu.SemaphoreType.REGULAR((GROUPS * (half - 1),)),
            pltpu.SemaphoreType.DMA((2 * layers, n)),
            pltpu.SemaphoreType.DMA((2 * layers, n)),
            pltpu.SemaphoreType.DMA((6 * CHUNKS,)),
            pltpu.SemaphoreType.DMA((6 * CHUNKS,)),
            pltpu.SemaphoreType.DMA((n,)),
            pltpu.SemaphoreType.DMA((n,)),
            pltpu.SemaphoreType.DMA((9,)),
        ]
    )
    out_shape = [
        jax.ShapeDtypeStruct((row_count, width), F32),
        jax.ShapeDtypeStruct((8, lanes), F32),
    ] + [jax.ShapeDtypeStruct((layers, blk, c), F32) for c in cols]
    return pl.pallas_call(
        functools.partial(backward_kernel, n, row_count),
        out_shape=out_shape,
        in_specs=[any_space] * 7 + [vmem] * 4 + [any_space] * GROUPS,
        out_specs=[any_space, vmem] + [any_space] * GROUPS,
        scratch_shapes=scratch,
        compiler_params=pltpu.CompilerParams(
            collective_id=1, has_side_effects=True, vmem_limit_bytes=67043328
        ),
        name="backward_layers",
    )(cotangent, *saved, gain_all, *tables, *full)


def unit_order(query, key, value):
    heads = key.shape[2] // HEAD_SIZE
    parts = []
    for u in range(heads):
        one = slice(u * HEAD_SIZE, (u + 1) * HEAD_SIZE)
        two = slice(2 * u * HEAD_SIZE, 2 * (u + 1) * HEAD_SIZE)
        parts += [query[:, :, two], key[:, :, one], value[:, :, one]]
    return jnp.concatenate(parts, axis=2)


def rope_tables(piece):
    lane = jnp.arange(UNIT, dtype=jnp.int32)
    inside = lane % HEAD_SIZE
    half = HEAD_SIZE // 2
    exponents = (inside % half).astype(F32) * (2.0 / HEAD_SIZE)
    positions = (piece * P_SIZE + jnp.arange(P_SIZE, dtype=jnp.int32)).astype(F32)
    angles = positions[:, None] * (rope_base**-exponents)[None, :]
    turned = (lane < 3 * HEAD_SIZE)[None, :]
    first = (inside < half)[None, :]
    sine = jnp.sin(angles)
    return (
        jnp.where(turned, jnp.cos(angles), 1.0),
        jnp.where(turned & first, -sine, 0.0),
        jnp.where(turned & ~first, sine, 0.0),
    )


def wide_rope_tables(positions, head_dim):
    half_dim = head_dim // 2
    exponents = jnp.arange(half_dim, dtype=jnp.float32) * (2.0 / head_dim)
    frequency = rope_base ** (-exponents)
    angles = positions[:, None] * frequency[None, :]
    return (jnp.cos(angles), jnp.sin(angles))


def apply_rotary(values, cosine_table, sine_table):
    half_dim = values.shape[-1] // 2
    first = values[..., :half_dim]
    second = values[..., half_dim:]
    cos_rows = cosine_table[:, None, :]
    sin_rows = sine_table[:, None, :]
    return jnp.concatenate(
        [first * cos_rows - second * sin_rows, second * cos_rows + first * sin_rows], axis=-1
    )


def rotate_back(grads, cosine_table, sine_table):
    half_dim = grads.shape[-1] // 2
    first = grads[..., :half_dim]
    second = grads[..., half_dim:]
    cos_rows = cosine_table[:, None, :]
    sin_rows = sine_table[:, None, :]
    return jnp.concatenate(
        [first * cos_rows + second * sin_rows, second * cos_rows - first * sin_rows], axis=-1
    )


def key_slab(kv_all, block, key_block, queries):
    seq_count, piece_len, kv_heads, query_groups, head_dim = queries.shape
    row_count = seq_count * piece_len
    slab = lax.dynamic_slice_in_dim(
        kv_all, block * (key_block * row_count), key_block * row_count, 0
    )
    slab = slab.reshape(key_block, seq_count, piece_len, 2, kv_heads, head_dim)
    slab = jnp.transpose(slab, (1, 0, 2, 3, 4, 5)).reshape(
        seq_count, key_block * piece_len, 2, kv_heads, head_dim
    )
    return (slab[:, :, 0], slab[:, :, 1])


def masked_scores(queries, keys, block, piece, key_block):
    piece_len = queries.shape[1]
    head_dim = queries.shape[4]
    key_len = key_block * piece_len
    query_pos = piece * piece_len + jnp.arange(piece_len, dtype=jnp.int32)
    key_pos = block * key_len + jnp.arange(key_len, dtype=jnp.int32)
    allowed = key_pos[None, :] <= query_pos[:, None]
    raw = jnp.einsum(
        "spkgd,stkd->skgpt", queries, keys, preferred_element_type=jnp.float32
    ) * head_dim ** (-0.5)
    return jnp.where(allowed, raw, big_negative)


def attend_forward(queries, kv_all, piece, key_block):
    seq_count, piece_len, kv_heads, query_groups, head_dim = queries.shape

    def step(block, carry):
        run_max, run_sum, total = carry
        keys, values = key_slab(kv_all, block, key_block, queries)
        scores = masked_scores(queries, keys, block, piece, key_block)
        new_max = jnp.maximum(run_max, jnp.max(scores, axis=-1))
        factor = jnp.exp(run_max - new_max)
        expo = jnp.exp(scores - new_max[..., None])
        run_sum = run_sum * factor + jnp.sum(expo, axis=-1)
        total = total * factor[..., None] + jnp.einsum(
            "skgpt,stkd->skgpd",
            expo.astype(jnp.bfloat16),
            values,
            preferred_element_type=jnp.float32,
        )
        return (new_max, run_sum, total)

    stats_shape = (seq_count, kv_heads, query_groups, piece_len)
    start = (
        jnp.full(stats_shape, big_negative, jnp.float32),
        jnp.zeros(stats_shape, jnp.float32),
        jnp.zeros(stats_shape + (head_dim,), jnp.float32),
    )
    run_max, run_sum, total = lax.fori_loop(0, piece // key_block + 1, step, start)
    return (total / run_sum[..., None], run_max + jnp.log(run_sum))


def attend_backward(queries, kv_all, piece, key_block, log_total, grad_heads, delta_rows, pieces):
    seq_count, piece_len, kv_heads, query_groups, head_dim = queries.shape
    row_count = seq_count * piece_len
    inv_sqrt = head_dim ** (-0.5)

    def step(block, carry):
        grad_query, terms = carry
        keys, values = key_slab(kv_all, block, key_block, queries)
        probs = jnp.exp(
            masked_scores(queries, keys, block, piece, key_block) - log_total[..., None]
        )
        grad_values = jnp.einsum(
            "skgpt,skgpd->stkd",
            probs.astype(jnp.bfloat16),
            grad_heads,
            preferred_element_type=jnp.float32,
        )
        grad_probs = jnp.einsum(
            "skgpd,stkd->skgpt", grad_heads, values, preferred_element_type=jnp.float32
        )
        grad_scores = (probs * (grad_probs - delta_rows[..., None])).astype(jnp.bfloat16)
        grad_query = (
            grad_query
            + jnp.einsum("skgpt,stkd->skgpd", grad_scores, keys, preferred_element_type=jnp.float32)
            * inv_sqrt
        )
        grad_keys = (
            jnp.einsum(
                "skgpt,spkgd->stkd", grad_scores, queries, preferred_element_type=jnp.float32
            )
            * inv_sqrt
        )
        paired = jnp.stack([grad_keys, grad_values], axis=2)
        paired = paired.reshape(seq_count, key_block, piece_len, 2 * kv_heads * head_dim)
        paired = jnp.transpose(paired, (1, 0, 2, 3)).reshape(
            key_block * row_count, 2 * kv_heads * head_dim
        )
        terms = lax.dynamic_update_slice_in_dim(terms, paired, block * (key_block * row_count), 0)
        return (grad_query, terms)

    start = (
        jnp.zeros(grad_heads.shape, jnp.float32),
        jnp.zeros((pieces * row_count, 2 * kv_heads * head_dim), jnp.float32),
    )
    return lax.fori_loop(0, piece // key_block + 1, step, start)


def exchange(value, axis, mask):
    size = lax.axis_size(axis)
    return lax.ppermute(value, axis, [(i, i ^ mask) for i in range(size)])


def gather_blocks(shard):
    half = lax.axis_size("gx") // 2
    near = jnp.concatenate(
        [shard] + [exchange(shard, "gx", 2 * k) for k in range(1, half)], axis=0
    )
    return (near, exchange(near, "gx", 1))


def in_features(pair, weights):
    return dot_nn(pair[0], weights[0]) + dot_nn(pair[1], weights[1])


def reduce_heads(lhs, weights):
    rows = lhs.shape[0] // 2
    width = weights[0].shape[0]
    away = jnp.concatenate([dot_nt(lhs[rows:], w).astype(BF16) for w in weights], axis=1)
    got = exchange(away, "gy", 1)
    own = [
        (dot_nt(lhs[:rows], w) + got[:, i * width : (i + 1) * width].astype(F32)).astype(BF16)
        for i, w in enumerate(weights)
    ]
    own = jnp.concatenate(own, axis=1)
    got = exchange(own, "gy", 2)
    total = (own.astype(F32) + got.astype(F32)).astype(BF16)
    other = exchange(total, "gy", 1)
    return tuple(
        jnp.concatenate(
            [total[:, i * width : (i + 1) * width], other[:, i * width : (i + 1) * width]], axis=0
        ).astype(F32)
        for i in range(2)
    )


def scatter_grad(pair, cols):
    half = lax.axis_size("gx") // 2
    got = exchange(dot_tn(pair[1], cols).astype(BF16), "gx", 1)
    near = dot_tn(pair[0], cols) + got.astype(F32)
    block = near.shape[0] // half
    low = near.astype(BF16)
    total = near[:block]
    for k in range(1, half):
        total = total + exchange(low[k * block : (k + 1) * block], "gx", 2 * k).astype(F32)
    return total


def norm_forward(hidden, gain):
    width = hidden[0].shape[1] * 2
    mean = sum(jnp.sum(h * h, axis=-1, keepdims=True) for h in hidden) / width
    inv_rms = lax.rsqrt(mean + norm_eps)
    normed = tuple((h * inv_rms * g).astype(BF16) for h, g in zip(hidden, gain))
    return (normed, inv_rms)


def norm_backward(grad_normed, hidden, inv_rms, gain):
    width = hidden[0].shape[1] * 2
    unit = [h * inv_rms for h in hidden]
    grad_unit = [d * g for d, g in zip(grad_normed, gain)]
    mean = sum(jnp.sum(d * u, axis=-1, keepdims=True) for d, u in zip(grad_unit, unit)) / width
    grad_hidden = tuple(inv_rms * (d - u * mean) for d, u in zip(grad_unit, unit))
    grad_gain = tuple(jnp.sum(d * u, axis=0) for d, u in zip(grad_normed, unit))
    return (grad_hidden, grad_gain)


def flip_if(bit, value, axis):
    return jnp.where(bit == 1, jnp.flip(value, axis), value)


def to_relative(value, me, core):
    n = lax.axis_size("gx")
    rows, width = value.shape
    bits = n.bit_length() - 1
    shape = (2, rows // 2) + (2,) * bits + (width // n,)
    value = value.reshape(shape)
    value = flip_if(core, value, 0)
    for b in range(bits):
        value = flip_if((me >> (bits - 1 - b)) & 1, value, 2 + b)
    value = value.reshape(rows, n // 2, 2, width // n)
    return tuple(value[:, :, i].reshape(rows, width // 2) for i in range(2))


def from_relative(pair, me, core):
    n = lax.axis_size("gx")
    rows, width = pair[0].shape[0], pair[0].shape[1] * 2
    bits = n.bit_length() - 1
    parts = [h.reshape(rows, n // 2, 1, width // n) for h in pair]
    value = jnp.concatenate(parts, axis=2)
    value = value.reshape((2, rows // 2) + (2,) * bits + (width // n,))
    value = flip_if(core, value, 0)
    for b in range(bits):
        value = flip_if((me >> (bits - 1 - b)) & 1, value, 2 + b)
    return value.reshape(rows, width)


def permute_program(
    inputs,
    gain_attn,
    w_query,
    w_key,
    value_projection,
    w_out,
    gain_ffn,
    w_gate,
    w_up,
    w_down,
    cotangent,
):
    pieces = lax.axis_size("gx")
    piece = lax.axis_index("gx")
    core = lax.axis_index("gy") & 1
    row_count = inputs.shape[0]
    seq_count = row_count // P_SIZE
    kv_heads = w_key.shape[2] // HEAD_SIZE
    query_groups = QUERY_HEADS // KEY_VALUE_HEADS
    q_width = w_query.shape[2]
    k_width = w_key.shape[2]
    ff = w_gate.shape[2]
    key_block = min(pieces, max(1, 512 // P_SIZE))
    positions = (piece * P_SIZE + jnp.arange(row_count, dtype=jnp.int32) % P_SIZE).astype(F32)
    cosine_table, sine_table = wide_rope_tables(positions, HEAD_SIZE)

    gains = jnp.concatenate([gain_attn, gain_ffn], axis=0)
    half = pieces // 2
    near = jnp.concatenate([gains] + [exchange(gains, "gx", 2 * k) for k in range(1, half)], axis=1)
    gains = (near.astype(F32), exchange(near, "gx", 1).astype(F32))

    def gain_of(row):
        return tuple(g[row : row + 1] for g in gains)

    layer_weights = []
    for layer in range(DECODER_LAYERS):
        layer_weights.append(
            (
                gather_blocks(
                    jnp.concatenate([w_query[layer], w_key[layer], value_projection[layer]], axis=1)
                ),
                gather_blocks(w_out[layer].T),
                gather_blocks(jnp.concatenate([w_gate[layer], w_up[layer]], axis=1)),
                gather_blocks(w_down[layer].T),
            )
        )

    hidden = to_relative(inputs.astype(F32), piece, core)
    records = []
    for layer in range(DECODER_LAYERS):
        qkv_mat, out_mat, ffn_mat, down_mat = layer_weights[layer]
        normed, inv_attn = norm_forward(hidden, gain_of(layer))
        qkv = in_features(normed, qkv_mat)
        query_lin = qkv[:, :q_width]
        key_linear = qkv[:, q_width : q_width + k_width]
        value_reduced = qkv[:, q_width + k_width :].astype(BF16)
        query_rotated = apply_rotary(
            query_lin.reshape(row_count, kv_heads * query_groups, HEAD_SIZE),
            cosine_table,
            sine_table,
        ).astype(BF16)
        key_rotated = apply_rotary(
            key_linear.reshape(row_count, kv_heads, HEAD_SIZE), cosine_table, sine_table
        ).astype(BF16)
        kv_local = jnp.concatenate([key_rotated.reshape(row_count, k_width), value_reduced], axis=1)
        kv_all = lax.all_gather(kv_local, "gx", axis=0, tiled=True)
        queries = query_rotated.reshape(seq_count, P_SIZE, kv_heads, query_groups, HEAD_SIZE)
        attended, log_total = attend_forward(queries, kv_all, piece, key_block)
        mixed = jnp.transpose(attended, (0, 3, 1, 2, 4)).reshape(row_count, q_width).astype(BF16)
        branch = reduce_heads(mixed, out_mat)
        middle = tuple(h + b for h, b in zip(hidden, branch))
        normed_ffn, inv_ffn = norm_forward(middle, gain_of(DECODER_LAYERS + layer))
        gate_up = in_features(normed_ffn, ffn_mat)
        gate, upward = gate_up[:, :ff], gate_up[:, ff:]
        inner = (jax.nn.silu(gate) * upward).astype(BF16)
        branch = reduce_heads(inner, down_mat)
        records.append(
            (
                hidden,
                normed,
                inv_attn,
                queries,
                kv_all,
                attended,
                log_total,
                mixed,
                middle,
                inv_ffn,
                normed_ffn,
                gate,
                upward,
                inner,
            )
        )
        hidden = tuple(m + b for m, b in zip(middle, branch))
    result = from_relative(hidden, piece, core)

    grad_hidden = to_relative(cotangent, piece, core)
    layer_grads = []
    gain_grads = {}
    for layer in reversed(range(DECODER_LAYERS)):
        (
            hidden,
            normed,
            inv_attn,
            queries,
            kv_all,
            attended,
            log_total,
            mixed,
            middle,
            inv_ffn,
            normed_ffn,
            gate,
            upward,
            inner,
        ) = records[layer]
        qkv_mat, out_mat, ffn_mat, down_mat = layer_weights[layer]
        grad_low = tuple(g.astype(BF16) for g in grad_hidden)
        grad_down = scatter_grad(grad_low, inner)
        grad_inner = in_features(grad_low, down_mat)
        sigmoid_gate = jax.nn.sigmoid(gate)
        grad_gate_low = (
            grad_inner * upward * sigmoid_gate * (1.0 + gate * (1.0 - sigmoid_gate))
        ).astype(BF16)
        grad_up_low = (grad_inner * gate * sigmoid_gate).astype(BF16)
        grad_ffn_low = jnp.concatenate([grad_gate_low, grad_up_low], axis=1)
        grad_ffn = scatter_grad(normed_ffn, grad_ffn_low)
        grad_middle_norm, gain_grads[DECODER_LAYERS + layer] = norm_backward(
            reduce_heads(grad_ffn_low, ffn_mat),
            middle,
            inv_ffn,
            gain_of(DECODER_LAYERS + layer),
        )
        grad_middle = tuple(g + d for g, d in zip(grad_hidden, grad_middle_norm))
        grad_low = tuple(g.astype(BF16) for g in grad_middle)
        grad_out = scatter_grad(grad_low, mixed)
        grad_mixed = in_features(grad_low, out_mat).astype(BF16)
        grad_heads = jnp.transpose(
            grad_mixed.reshape(seq_count, P_SIZE, kv_heads, query_groups, HEAD_SIZE),
            (0, 2, 3, 1, 4),
        )
        delta_rows = jnp.sum(grad_heads.astype(F32) * attended, axis=-1)
        grad_queries, kv_terms = attend_backward(
            queries, kv_all, piece, key_block, log_total, grad_heads, delta_rows, pieces
        )
        kv_grad = lax.psum_scatter(
            kv_terms.astype(BF16), "gx", scatter_dimension=0, tiled=True
        ).astype(F32).reshape(row_count, 2, kv_heads, HEAD_SIZE)
        grad_key_low = (
            rotate_back(kv_grad[:, 0], cosine_table, sine_table)
            .reshape(row_count, k_width)
            .astype(BF16)
        )
        grad_value_low = kv_grad[:, 1].reshape(row_count, k_width).astype(BF16)
        grad_query_rows = jnp.transpose(grad_queries, (0, 3, 1, 2, 4)).reshape(
            row_count, kv_heads * query_groups, HEAD_SIZE
        )
        grad_query_low = (
            rotate_back(grad_query_rows, cosine_table, sine_table)
            .reshape(row_count, q_width)
            .astype(BF16)
        )
        grad_qkv_low = jnp.concatenate([grad_query_low, grad_key_low, grad_value_low], axis=1)
        grad_qkv = scatter_grad(normed, grad_qkv_low)
        grad_in_norm, gain_grads[layer] = norm_backward(
            reduce_heads(grad_qkv_low, qkv_mat), hidden, inv_attn, gain_of(layer)
        )
        grad_hidden = tuple(g + d for g, d in zip(grad_middle, grad_in_norm))
        layer_grads.append((grad_qkv, grad_out, grad_ffn, grad_down))
    layer_grads = layer_grads[::-1]
    gain_near, gain_far = [
        jnp.stack([gain_grads[row][side] for row in range(2 * DECODER_LAYERS)]) for side in range(2)
    ]
    near = gain_near + exchange(gain_far, "gx", 1)
    block = near.shape[1] // half
    gain_total = near[:, :block]
    for k in range(1, half):
        gain_total = gain_total + exchange(near[:, k * block : (k + 1) * block], "gx", 2 * k)
    qkv, out, ffn, down = [jnp.stack([g[i] for g in layer_grads]) for i in range(4)]
    return (
        result,
        from_relative(grad_hidden, piece, core),
        gain_total[:DECODER_LAYERS],
        qkv[:, :, :q_width],
        qkv[:, :, q_width : q_width + k_width],
        qkv[:, :, q_width + k_width :],
        jnp.swapaxes(out, 1, 2),
        gain_total[DECODER_LAYERS:],
        ffn[:, :, :ff],
        ffn[:, :, ff:],
        jnp.swapaxes(down, 1, 2),
    )


def per_device(
    inputs,
    gain_attn,
    w_query,
    w_key,
    value_projection,
    w_out,
    gain_ffn,
    w_gate,
    w_up,
    w_down,
    cotangent,
):
    n = lax.axis_size("gx")
    piece = lax.axis_index("gx")
    if inputs.shape[0] // P_SIZE * (w_key.shape[2] // HEAD_SIZE) != n:
        return permute_program(
            inputs,
            gain_attn,
            w_query,
            w_key,
            value_projection,
            w_out,
            gain_ffn,
            w_gate,
            w_up,
            w_down,
            cotangent,
        )
    gains = jnp.concatenate([gain_attn, gain_ffn], axis=0).astype(F32)
    lanes = -(-gains.shape[1] // 128) * 128
    gains = jnp.pad(gains, ((0, 8 - gains.shape[0]), (0, lanes - gains.shape[1])))
    shards = (
        unit_order(w_query, w_key, value_projection),
        jnp.swapaxes(w_out, 1, 2),
        w_gate,
        w_up,
        jnp.swapaxes(w_down, 1, 2),
    )
    tables = rope_tables(piece)
    outs = forward(n, inputs, gains, tables, shards)
    result, hidden, middle, gate, up, unit, mixed, gain_all = outs[:8]
    saved = (hidden, middle, gate, up, unit, mixed)
    grads = backward(n, cotangent, saved, gain_all, tables, outs[8:])
    grad_inputs, grad_gain, qkv, out, grad_gate, grad_up, down = grads
    heads = w_key.shape[2] // HEAD_SIZE
    parts = [qkv[:, :, u * UNIT : (u + 1) * UNIT] for u in range(heads)]
    size = HEAD_SIZE
    grad_gain = grad_gain[:, : gain_attn.shape[1]]
    return (
        result,
        grad_inputs,
        grad_gain[:DECODER_LAYERS],
        jnp.concatenate([p[:, :, : 2 * size] for p in parts], axis=2),
        jnp.concatenate([p[:, :, 2 * size : 3 * size] for p in parts], axis=2),
        jnp.concatenate([p[:, :, 3 * size :] for p in parts], axis=2),
        jnp.swapaxes(out, 1, 2),
        grad_gain[DECODER_LAYERS : 2 * DECODER_LAYERS],
        grad_gate,
        grad_up,
        jnp.swapaxes(down, 1, 2),
    )


def solution(mesh):
    return jax.shard_map(
        per_device,
        mesh=mesh,
        in_specs=(
            P("gx", None),
            P(None, "gx"),
            P(None, "gx", "gy"),
            P(None, "gx", "gy"),
            P(None, "gx", "gy"),
            P(None, "gy", "gx"),
            P(None, "gx"),
            P(None, "gx", "gy"),
            P(None, "gx", "gy"),
            P(None, "gy", "gx"),
            P("gx", None),
        ),
        out_specs=(
            P("gx", None),
            P("gx", None),
            P(None, "gx"),
            P(None, "gx", "gy"),
            P(None, "gx", "gy"),
            P(None, "gx", "gy"),
            P(None, "gy", "gx"),
            P(None, "gx"),
            P(None, "gx", "gy"),
            P(None, "gx", "gy"),
            P(None, "gy", "gx"),
        ),
        check_vma=False,
    )
```
